256 devices in a mesh: rec: 64 (over z, y, core), vocab: 4 (over x).
Axes of the slice: x: 4, y: 4, z: 8, core: 2. Of those that a mesh axis runs over, the one named last changes fastest.
Arguments:
- features: bfloat16 [256, 192, 1280], P('rec'), may hold values from -1000 to 1000
- head_weight: bfloat16 [1280, 32768], P(None, ('vocab', 'rec')), may hold values from -0.15625 to 0.15625
- labels: int32 [256, 128], P('rec'), may hold values from 0 to 32767
- audio_len: int32 [256], P(('rec', 'vocab')), may hold values from 1 to 192, as said below
- transcript_len: int32 [256], P(('rec', 'vocab')), may hold values from 1 to 128
Outputs:
- label_logprob: float32 [256, 192, 128], P(('rec', 'vocab'))
- path_score: float32 [256], P(('rec', 'vocab'))
The draws below stay inside these ranges and needn't reach their ends.
Inputs may be any that keep to these rules, and one draw needn't show every extreme that they name: `audio_len`: each recording has at least as many frames in use as its transcript has labels.
All inputs are finite; a program needn't handle non-finite values.
Results may differ from the reference program's by a relative error of at most 0.00055.
Values may be sent and summed in bfloat16 or wider, within the bound.
No kernel may reach another device: no remote copies, remote signals or barrier semaphores. Data moves between devices by JAX's collectives and lax.ppermute only.
A program may use at most 128 MiB of HBM per device.

```python
import math
import jax
import jax.numpy as jnp
import numpy as np
from jax import lax

D = 1280
VOCAB = 32768
FRAMES = 192
LABELS = 128
REC = 256


def draw_features(key, part):
    key_base = jax.random.fold_in(key, 0)
    values = jnp.clip(jax.random.normal(key_base, (REC, FRAMES, D), jnp.float32), -6.0, 6.0)
    values = values * 3.0
    return values.astype(jnp.bfloat16)


def length_pair(key):
    inner = jax.random.fold_in(key, 7)
    key_text, key_audio = jax.random.split(inner)
    text_len = jax.random.randint(key_text, (REC,), 1, LABELS + 1)
    text_len = text_len.at[1].set(LABELS)
    audio_len = jax.random.randint(key_audio, (REC,), text_len, FRAMES + 1)
    audio_len = jnp.maximum(audio_len, text_len)
    audio_len = audio_len.at[0].set(FRAMES)
    return (audio_len.astype(jnp.int32), text_len.astype(jnp.int32))


def draw_audio_len(key, part):
    return length_pair(key)[0]


def draw_transcript_len(key, part):
    return length_pair(key)[1]


def place_ends(array, rng, least, top_value):
    longest = array.shape.index(max(array.shape))
    spots = []
    for shift in (0, 1):
        where = [jax.random.randint(jax.random.fold_in(rng, axis), (), 0, length) for axis, length in enumerate(array.shape)]
        where[longest] = (where[longest] + shift) % array.shape[longest]
        spots.append(tuple(where))
    return array.at[spots[0]].set(least).at[spots[1]].set(top_value)


def block_levels(stream_key, dims, pieces, least, high):
    gain, own = 1.0, jax.random.fold_in(stream_key, 6)
    for axis_at, shards_of in pieces:
        steps = jnp.exp(jax.random.uniform(jax.random.fold_in(own, axis_at), (shards_of,), jnp.float32, least / len(pieces), high / len(pieces)))
        gain = gain * jnp.repeat(steps, dims[axis_at] // shards_of).reshape([-1 if axis == axis_at else 1 for axis in range(len(dims))])
    return gain


def cumulative_ranks(number_of, skew):
    portions = [(1 << 20) // math.isqrt(grade ** skew) + 1 for grade in range(1, number_of + 1)]
    deviation = 1 + sum(portions) // (1 << 30)
    return np.cumsum(np.array([max(1, weight // deviation) for weight in portions]))


def ranked_ids(rng, shape, amount, lean):
    grid = cumulative_ranks(amount, lean)
    lot = jax.random.randint(jax.random.fold_in(rng, 1), shape, 0, int(grid[amount - 1]))
    grade = jnp.searchsorted(jnp.asarray(grid, jnp.int32), lot, side="right")
    return jax.random.permutation(jax.random.fold_in(rng, 2), amount)[grade].astype(jnp.int32)


def normal_values(key, shape, width, reach, shards=(), dtype=jnp.bfloat16):
    drawn = jax.random.normal(key, shape, jnp.float32) * width
    if len(shards) > 0:
        drawn = block_levels(key, shape, shards, -0.22, 0.18) * drawn
    return jnp.clip(drawn, min=-reach, max=reach).astype(dtype)


def setup_inputs(seed: int = 0) -> dict:
    splits = jax.random.split(jax.random.key(seed), 6)
    return {
        "features": draw_features(jax.random.fold_in(splits[5], 71), 0),
        "head_weight": normal_values(splits[1], (D, VOCAB), D ** -0.5, 0.15625, ((1, 256),)),
        "labels": place_ends(ranked_ids(splits[2], (REC, LABELS), VOCAB, 2), jax.random.fold_in(splits[2], 3), 0, VOCAB - 1).astype(jnp.int32),
        "audio_len": draw_audio_len(jax.random.fold_in(splits[5], 71), 0),
        "transcript_len": draw_transcript_len(jax.random.fold_in(splits[5], 71), 0),
    }


negative_fill = -1e30


def viterbi(log_prob, audio_len, transcript_len):
    rec_count, frames, slots = log_prob.shape
    states = lax.iota(jnp.int32, slots)[None, :]
    target = states == (transcript_len[:, None] - 1)
    initial = jnp.where(states == 0, log_prob[:, 0, :], negative_fill)
    best_end = jnp.where(audio_len == 1, jnp.sum(jnp.where(target, initial, 0.0), 1), 0.0)

    def advance(frame_index, carry):
        current, best_end = carry
        shifted = jnp.concatenate([jnp.full_like(current[:, :1], negative_fill), current[:, :-1]], 1)
        emitted = lax.dynamic_index_in_dim(log_prob, frame_index, 1, keepdims=False)
        current = jnp.maximum(current, shifted) + emitted
        reached = jnp.sum(jnp.where(target, current, 0.0), 1)
        best_end = jnp.where(audio_len - 1 == frame_index, reached, best_end)
        return current, best_end

    current, best_end = lax.fori_loop(1, frames, advance, (initial, best_end))
    return best_end


def reference(features, head_weight, labels, audio_len, transcript_len):
    def per_recording(inputs):
        frame_feats, label_ids = inputs
        logits = jnp.dot(frame_feats, head_weight, preferred_element_type=jnp.float32)
        row_top = jnp.max(logits, 1)
        log_norm = row_top + jnp.log(jnp.sum(jnp.exp(logits - row_top[:, None]), 1))
        picked = jnp.take(logits.astype(jnp.bfloat16), label_ids, axis=1).astype(jnp.float32)
        return picked - log_norm[:, None]

    log_prob = lax.map(per_recording, (features, labels))
    return log_prob, viterbi(log_prob, audio_len, transcript_len)
```

```python
import functools

import jax
import jax.numpy as jnp
import numpy as np
from jax import lax
from jax.experimental import pallas as pl
from jax.experimental.pallas import tpu as pltpu
from jax.sharding import PartitionSpec as P

negative_fill = -1e30
NZ, NY = 8, 4
TILE = 256
BLOCK = 512
ANY = pl.BlockSpec(memory_space=pl.ANY)
VMEM = pl.BlockSpec(memory_space=pltpu.VMEM)
SMEM = pl.BlockSpec(memory_space=pltpu.SMEM)


def rec_index(z, y, core):
    return ((z % NZ) * NY + y % NY) * 2 + core


def moves(step0=None, step1=None, swap=0):
    pairs = []
    for core, step in ((0, step0), (1, step1)):
        if step is None:
            continue
        for z in range(NZ):
            for y in range(NY):
                pairs.append(
                    (rec_index(z, y, core), rec_index(z + step[0], y + step[1], core ^ swap))
                )
    return pairs


ZP, ZM, YP, YM = (1, 0), (-1, 0), (0, 1), (0, -1)


def place_tables():
    first = [(0, 0), (-1, 0), (1, 0), (-2, 0)]
    second = [(2, 0), (-3, 0), (3, 0), (4, 0)]
    table = np.zeros((2, NZ * NY), np.int32)
    blocks0 = [(first, 0), (first, -1), (first, 1), (first, -2), (second, -1), (second, 1), (second, 2), (second, 0)]
    for b, (subs, dy) in enumerate(blocks0):
        for s, (dz, _) in enumerate(subs):
            table[0, (dz % NZ) * NY + dy % NY] = b * 4 + s
    for b, dz in enumerate([0, -1, 1, -2, -3, 2, 3, 4]):
        for s, dy in enumerate([0, -1, 1, -2]):
            table[1, (dz % NZ) * NY + dy % NY] = b * 4 + s
    return table


def block_update(w_vmem, f_vmem, f_sems, f_copies, l_ref, m_ref, s_ref, fresh):
    tiles = f_vmem.shape[0]

    def tile_step(t, _):
        for k, copy in enumerate(f_copies):

            @pl.when(t == k * (tiles // len(f_copies)))
            def _(copy=copy):
                copy.wait()

        tile = lax.dot_general(
            w_vmem[...], f_vmem[t], (((1,), (1,)), ((), ())), preferred_element_type=jnp.float32
        )
        l_ref[2 * t] = tile[:, :128]
        l_ref[2 * t + 1] = tile[:, 128:]
        cube = tile.reshape(BLOCK // 8, 8, TILE)
        top = jnp.max(cube, 0)
        if not fresh:
            old = m_ref[t]
            top = jnp.maximum(top, old)
        total = jnp.sum(jnp.exp(cube - top[None]), 0)
        if not fresh:
            total = total + s_ref[t] * jnp.exp(old - top)
        m_ref[t] = top
        s_ref[t] = total
        return 0

    lax.fori_loop(0, tiles, tile_step, 0)


def take_rows(block, bounds, entries, l_ref, p_ref):
    def one(k, _):
        entry = entries[k]
        row = entry // 1024
        item = entry % 1024
        window = (item // 128) * 3 // 2
        p_ref[0, pl.ds(item, 1), :] = l_ref[window, pl.ds(row, 1), :]
        p_ref[1, pl.ds(item, 1), :] = l_ref[window + 1, pl.ds(row, 1), :]
        return 0

    lax.fori_loop(bounds[block], bounds[block + 1], one, 0)


def start_features(fa, fb, f_vmem, sems):
    half = f_vmem.shape[0] // 2
    copies = []
    for k, ref in enumerate((fa, fb)):
        copy = pltpu.make_async_copy(ref, f_vmem.at[pl.ds(k * half, half)], sems.at[k])
        copy.start()
        copies.append(copy)
    return copies


def first_kernel(bounds, entries, w, fa, fb, m_out, s_out, p_out, f_vmem, l_ref, sems):
    copies = start_features(fa, fb, f_vmem, sems)
    p_out[...] = jnp.zeros_like(p_out)
    block_update(w, f_vmem, sems, copies, l_ref, m_out, s_out, True)
    take_rows(0, bounds, entries, l_ref, p_out)


def next_kernel(block, bounds, entries, w, fa, fb, m_in, s_in, p_in, m_out, s_out, p_out, f_vmem, l_ref, sems):
    copies = start_features(fa, fb, f_vmem, sems)
    m_out[...] = m_in[...]
    s_out[...] = s_in[...]
    p_out[...] = p_in[...]
    block_update(w, f_vmem, sems, copies, l_ref, m_out, s_out, False)
    take_rows(block, bounds, entries, l_ref, p_out)


def last_kernel(where, bounds, entries, w0, w1a, w1b, fa, fb, m_in, s_in, p_in, *rest):
    outs, (m_ref, s_ref, p_ref, w_vmem, f_vmem, l_ref, lse_ref, sems, w_sems) = rest[:8], rest[8:]
    copies = start_features(fa, fb, f_vmem, sems)
    place, core = where[0], where[1]

    @pl.when(core == 0)
    def _():
        copy = pltpu.make_async_copy(w0, w_vmem, w_sems.at[0])
        copy.start()
        copy.wait()

    @pl.when(core == 1)
    def _():
        half = BLOCK // 2
        one = pltpu.make_async_copy(w1a, w_vmem.at[pl.ds(0, half)], w_sems.at[0])
        two = pltpu.make_async_copy(w1b, w_vmem.at[pl.ds(half, half)], w_sems.at[1])
        one.start()
        two.start()
        one.wait()
        two.wait()

    m_ref[...] = m_in[...]
    s_ref[...] = s_in[...]
    p_ref[...] = p_in[...]
    block_update(w_vmem, f_vmem, sems, copies, l_ref, m_ref, s_ref, False)
    take_rows(BLOCKS - 1, bounds, entries, l_ref, p_ref)
    for t in range(m_ref.shape[0]):
        top = jnp.max(m_ref[t], 0, keepdims=True)
        total = jnp.sum(s_ref[t] * jnp.exp(m_ref[t] - top), 0, keepdims=True)
        value = jnp.broadcast_to(top + jnp.log(total), (8, TILE))
        lse_ref[2 * t] = value[:, :128]
        lse_ref[2 * t + 1] = value[:, 128:]
    for half in range(2):
        for step in range(4):
            rec = half * 4 + (place + step) % 4
            out = outs[half * 4 + step]
            shift = (TILE - 64 * (rec % 2)) % TILE
            slots = pl.ds(pl.multiple_of(rec * 128, 128), 128)
            rows = jnp.concatenate([p_ref[0, slots, :], p_ref[1, slots, :]], 1)
            out[0:128, :] = pltpu.roll(rows, shift, 1).astype(jnp.bfloat16)
            window = rec * 3 // 2
            value = jnp.concatenate([lse_ref[window], lse_ref[window + 1]], 1)
            value = pltpu.roll(value, shift, 1)
            high = value.astype(jnp.bfloat16).astype(jnp.float32)
            middle = (value - high).astype(jnp.bfloat16).astype(jnp.float32)
            low = value - high - middle
            line = lax.broadcasted_iota(jnp.int32, (8, TILE), 0)
            parts = jnp.where(line == 0, high, jnp.where(line == 1, middle, jnp.where(line == 2, low, 0.0)))
            parts = jnp.concatenate([parts, jnp.zeros_like(parts)], 0)
            out[128:144, :] = parts.astype(jnp.bfloat16)


DEPTH = 8


def align_kernel(lengths, *refs):
    parts, (logprob, path, turned, scores) = refs[:8], refs[8:]
    frames = logprob.shape[0]
    picked = parts[0][0:128, :].astype(jnp.float32)
    for part in parts[1:]:
        picked = picked + part[0:128, :].astype(jnp.float32)
    norms = []
    for part in parts:
        lines = part[128:144, :].astype(jnp.float32)
        norms.append(lines[0:1] + lines[1:2] + lines[2:3])
    top = functools.reduce(jnp.maximum, norms)
    norm = top + jnp.log(sum(jnp.exp(value - top) for value in norms))
    table = (picked - norm).T[:frames]
    logprob[...] = table
    lanes = lax.broadcasted_iota(jnp.int32, (1, 128), 1)
    for d in range(DEPTH):
        turned[d] = table if d == 0 else pltpu.roll(table, d, 1)

    def advance(score, first, count):
        copies = [score] + [jnp.where(lanes < d, negative_fill, pltpu.roll(score, d, 1)) for d in range(1, count + 1)]
        for i in range(count):
            for d in range(count - i):
                emitted = turned[d, pl.ds(first + i, 1), :]
                copies[d] = jnp.maximum(copies[d], copies[d + 1]) + emitted
            scores[pl.ds(first + i, 1), :] = copies[0]
        return copies[0]

    score = jnp.where(lanes == 0, table[0:1], negative_fill)
    scores[0:1, :] = score
    score = advance(score, 1, DEPTH - 1)
    lax.fori_loop(1, frames // DEPTH, lambda b, now: advance(now, pl.multiple_of(b * DEPTH, DEPTH), DEPTH), score)
    final = scores[pl.ds(lengths[0] - 1, 1), :]
    hit = jnp.sum(jnp.where(lanes == lengths[1] - 1, final, 0.0), 1, keepdims=True)
    path[...] = jnp.broadcast_to(hit, path.shape)


BLOCKS = 8


def label_entries(labels, vocab_index, z, y, core):
    flat = labels.reshape(-1)
    local = flat % (NZ * NY * 256)
    owner = local // 128
    owner_core = owner % 2
    dy = (owner // 2 - y) % NY
    dz = (owner // (2 * NY) - z) % NZ
    table = jnp.where(core == 0, jnp.asarray(place_tables()[0]), jnp.asarray(place_tables()[1]))
    kinds = lax.iota(jnp.int32, NZ * NY)
    position = jnp.sum(jnp.where((dz * NY + dy)[:, None] == kinds[None], table[None], 0), 1)
    mine = (flat // (NZ * NY * 256) == vocab_index) & (owner_core == core)
    block = jnp.where(mine, position // 4, BLOCKS)
    row = position % 4 * 128 + local % 128
    ids = lax.iota(jnp.int32, flat.shape[0])
    sort_key = block * 1024 + ids
    rank = jnp.sum((sort_key[None, :] < sort_key[:, None]).astype(jnp.int32), 1)
    value = row * 1024 + ids
    entries = jnp.sum(jnp.where(rank[:, None] == ids[None, :], value[:, None], 0), 0)
    steps = lax.iota(jnp.int32, 16)
    bounds = jnp.sum((block[:, None] < steps[None, :]).astype(jnp.int32), 0)
    return bounds, entries


def body(features, head_weight, labels, audio_len, transcript_len):
    rec_dev, frames, width = features.shape
    rows = rec_dev * frames
    vocab_index = lax.axis_index("vocab")
    rec = lax.axis_index("rec")
    core, y, z = rec % 2, rec // 2 % NY, rec // (2 * NY)
    swap = moves((0, 0), (0, 0), 1)

    def send(array, step0, step1):
        return lax.ppermute(array, "rec", moves(step0, step1))

    own = head_weight.T
    a1 = send(own, ZP, YP)
    a2 = send(own, ZM, YM)
    tiles = rows // TILE
    fa = features.reshape(tiles, TILE, width)
    fb = lax.ppermute(features, "rec", swap).reshape(tiles, TILE, width)
    other_labels = lax.ppermute(labels, "rec", swap)
    bounds, entries = label_entries(jnp.concatenate([labels, other_labels]), vocab_index, z, y, core)
    a3 = send(a1, ZP, YP)
    c1 = jnp.concatenate([own, a1, a2, a3])
    b1 = send(c1, YP, ZP)
    b2 = send(c1, YM, ZM)
    a4 = send(a2, ZM, None)
    a5 = send(a3, ZP, None)
    a6 = send(a4, ZM, None)
    a7 = send(a6, ZM, None)
    c2 = jnp.concatenate([a4, a5, a6, a7])
    b3 = send(b1, YP, ZP)
    b4 = send(jnp.where(core == 0, c2, b3), YP, ZP)
    b5 = send(jnp.where(core == 0, c2, b2), YM, ZM)
    b6 = send(b5, YM, ZM)
    half = BLOCK // 2
    b7 = send(b4[:half], None, ZP)
    b8 = send(b6[half:], None, ZM)

    f32 = jnp.float32
    state = (
        jax.ShapeDtypeStruct((2 * tiles, 8, TILE), f32),
        jax.ShapeDtypeStruct((2 * tiles, 8, TILE), f32),
        jax.ShapeDtypeStruct((2, 8 * 128, 128), f32),
    )
    scratch = [
        pltpu.VMEM((2 * tiles, TILE, width), jnp.bfloat16),
        pltpu.VMEM((4 * tiles, BLOCK, 128), f32),
    ]
    cost = pl.CostEstimate(
        flops=2 * 2 * rows * BLOCK * width, bytes_accessed=8_000_000, transcendentals=2 * rows * BLOCK
    )
    carried = pl.pallas_call(
        first_kernel,
        out_shape=state,
        in_specs=[SMEM, SMEM, VMEM, ANY, ANY],
        out_specs=[VMEM] * 3,
        scratch_shapes=[*scratch, pltpu.SemaphoreType.DMA((2,))],
        cost_estimate=cost,
    )(bounds, entries, c1, fa, fb)
    for number, block in enumerate((b1, b2, b3, b4, b5, b6)):
        carried = pl.pallas_call(
            functools.partial(next_kernel, number + 1),
            out_shape=state,
            in_specs=[SMEM, SMEM, VMEM, ANY, ANY, VMEM, VMEM, VMEM],
            out_specs=[VMEM] * 3,
            scratch_shapes=[*scratch, pltpu.SemaphoreType.DMA((2,))],
            cost_estimate=cost,
        )(bounds, entries, block, fa, fb, *carried)
    payload = jax.ShapeDtypeStruct((144, TILE), jnp.bfloat16)
    sent = pl.pallas_call(
        last_kernel,
        out_shape=[payload] * 8,
        in_specs=[SMEM, SMEM, SMEM, ANY, ANY, ANY, ANY, ANY, VMEM, VMEM, VMEM],
        out_specs=[VMEM] * 8,
        scratch_shapes=[
            *(pltpu.VMEM(leaf.shape, leaf.dtype) for leaf in state),
            pltpu.VMEM((BLOCK, width), jnp.bfloat16),
            *scratch,
            pltpu.VMEM((4 * tiles, 8, 128), f32),
            pltpu.SemaphoreType.DMA((2,)),
            pltpu.SemaphoreType.DMA((2,)),
        ],
        cost_estimate=cost,
    )(jnp.stack([vocab_index, core]), bounds, entries, c2, b7, b8, fa, fb, *carried)
    vocabs = lax.axis_size("vocab")
    groups = lax.axis_size("rec")
    got = []
    for side in range(2):
        for step in range(vocabs):
            part = sent[side * 4 + step]
            if side or step:
                pairs = [
                    (g * vocabs + v, (g ^ side) * vocabs + (v + step) % vocabs)
                    for g in range(groups)
                    for v in range(vocabs)
                ]
                part = lax.ppermute(part, ("rec", "vocab"), pairs)
            got.append(part)
    log_prob, path = pl.pallas_call(
        align_kernel,
        out_shape=[jax.ShapeDtypeStruct((frames, 128), f32), jax.ShapeDtypeStruct((8, 128), f32)],
        in_specs=[SMEM, *([VMEM] * 8)],
        out_specs=[VMEM] * 2,
        scratch_shapes=[pltpu.VMEM((DEPTH, frames, 128), f32), pltpu.VMEM((frames, 128), f32)],
    )(jnp.concatenate([audio_len, transcript_len]), *got)
    return log_prob[None], path[0, :1]


def solution(mesh):
    placed = (
        P("rec", None, None),
        P(None, ("vocab", "rec")),
        P("rec", None),
        P(("rec", "vocab")),
        P(("rec", "vocab")),
    )
    return jax.shard_map(
        body,
        mesh=mesh,
        in_specs=placed,
        out_specs=(P(("rec", "vocab"), None, None), P(("rec", "vocab"))),
        check_vma=False,
    )
```

```python
import functools

import jax
import jax.numpy as jnp
import numpy as np
from jax import lax
from jax.experimental import pallas as pl
from jax.experimental.pallas import tpu as pltpu
from jax.sharding import PartitionSpec as P

negative_fill = -1e30
NZ, NY = 8, 4
TILE = 256
BLOCK = 512
PAIRS = 4
WINDOWS = 12
EARLY = 512
ANY = pl.BlockSpec(memory_space=pl.ANY)
VMEM = pl.BlockSpec(memory_space=pltpu.VMEM)
SMEM = pl.BlockSpec(memory_space=pltpu.SMEM)
LOWEST = -3.0e38


def rec_index(z, y, core):
    return ((z % NZ) * NY + y % NY) * 2 + core


def moves(step0=None, step1=None):
    pairs = []
    for core, step in ((0, step0), (1, step1)):
        if step is None:
            continue
        for z in range(NZ):
            for y in range(NY):
                pairs.append((rec_index(z, y, core), rec_index(*step(z, y, core))))
    return pairs


def other_core(z, y, core):
    return z, y, 1 - core


def up(z, y, core):
    return z + 1, y, core


def down(z, y, core):
    return z - 1, y, core


def mirror(z, y, core):
    return z, 3 - y, core


def beside(z, y, core):
    return z, y ^ 1, core


def place_table():
    table = np.full((2, 2 * NZ), 2 * PAIRS, np.int32)
    order0 = [(-1, 0), (-2, 0), (-1, 1), (-3, 0), (-4, 0), (-2, 1), (-3, 1), (-4, 1)]
    order1 = [(1, 0), (2, 0), (1, 1), (3, 0), (2, 1), (0, 0), (3, 1), (0, 1)]
    for core, order in ((0, order0), (1, order1)):
        for place, (dz, far) in enumerate(order):
            table[core, far * NZ + dz % NZ] = place
    return table


def score_tiles(w_ref, pair, f_ref, first_tile, l_ref, m_ref, s_ref):
    def step(t, _):
        rows = f_ref[pl.ds(pl.multiple_of(t * TILE, TILE), TILE), :]
        tile = lax.dot_general(
            w_ref[pair], rows, (((1,), (1,)), ((), ())), preferred_element_type=jnp.float32
        )
        at = first_tile + t
        l_ref[2 * at] = tile[:, :128]
        l_ref[2 * at + 1] = tile[:, 128:]
        cube = tile.reshape(BLOCK // 8, 8, TILE)
        old = m_ref[at]
        top = jnp.maximum(jnp.max(cube, 0), old)
        s_ref[at] = s_ref[at] * jnp.exp(old - top) + jnp.sum(jnp.exp(cube - top[None]), 0)
        m_ref[at] = top
        return 0

    lax.fori_loop(0, f_ref.shape[0] // TILE, step, 0)


def take_rows(pair, which, bounds, entries, l_ref, p_ref, early=None):
    def one(k, _):
        entry = entries[which, k]
        row = entry // 1024
        item = entry % 1024
        for side in range(2):
            window = (item // 128) * 3 // 2 + side

            def copy(window=window, side=side):
                p_ref[side, pl.ds(item, 1), :] = l_ref[window, pl.ds(row, 1), :]

            if early is None:
                copy()
            else:
                inside = window % (WINDOWS // 2) < EARLY // 128
                pl.when(inside if early else jnp.logical_not(inside))(copy)
        return 0

    lax.fori_loop(bounds[which, pair], bounds[which, pair + 1], one, 0)


def fill_pair(w_ref, pair, one, two):
    w_ref[pair, 0 : BLOCK // 2] = one[...]
    w_ref[pair, BLOCK // 2 : BLOCK] = two[...]


def first_kernel(bounds, entries, one, two, fa, fb, m, s, p, w_ref, l_ref):
    m[...] = jnp.full_like(m, LOWEST)
    s[...] = jnp.zeros_like(s)
    p[...] = jnp.zeros_like(p)
    fill_pair(w_ref, 0, one, two)
    score_tiles(w_ref, 0, fa, 0, l_ref, m, s)
    score_tiles(w_ref, 0, fb, 3, l_ref, m, s)
    take_rows(0, 0, bounds, entries, l_ref, p)


def second_kernel(bounds, entries, one, two, fa, fb, m_in, s_in, p_in, m, s, p, w_ref, l_ref):
    m[...] = m_in[...]
    s[...] = s_in[...]
    p[...] = p_in[...]
    fill_pair(w_ref, 0, one, two)
    score_tiles(w_ref, 0, fa, 0, l_ref, m, s)
    score_tiles(w_ref, 0, fb, 3, l_ref, m, s)
    take_rows(1, 0, bounds, entries, l_ref, p)


def third_kernel(bounds, entries, *refs):
    blocks, (fa, fb, ga, gb, m_in, s_in, p_in), (m, s, p, mb, sb, pb, w_ref, l_ref) = refs[:6], refs[6:13], refs[13:]
    m[...] = m_in[...]
    s[...] = s_in[...]
    p[...] = p_in[...]
    mb[...] = jnp.full_like(mb, LOWEST)
    sb[...] = jnp.zeros_like(sb)
    pb[...] = jnp.zeros_like(pb)
    for pair in range(3):
        fill_pair(w_ref, pair, *blocks[2 * pair : 2 * pair + 2])
    score_tiles(w_ref, 2, fa, 0, l_ref, m, s)
    score_tiles(w_ref, 2, fb, 3, l_ref, m, s)
    take_rows(2, 0, bounds, entries, l_ref, p)

    def over(pair, _):
        score_tiles(w_ref, pair, ga, 0, l_ref, mb, sb)
        score_tiles(w_ref, pair, gb, 3, l_ref, mb, sb)
        take_rows(pair, 1, bounds, entries, l_ref, pb, True)
        return 0

    lax.fori_loop(0, 3, over, 0)


def split_parts(value):
    high = value.astype(jnp.bfloat16).astype(jnp.float32)
    middle = (value - high).astype(jnp.bfloat16).astype(jnp.float32)
    low = value - high - middle
    line = lax.broadcasted_iota(jnp.int32, value.shape, 0)
    parts = jnp.where(line == 0, high, jnp.where(line == 1, middle, jnp.where(line == 2, low, 0.0)))
    return jnp.concatenate([parts, jnp.zeros_like(parts)], 0).astype(jnp.bfloat16)


def joined_parts(lines):
    lines = lines.astype(jnp.float32)
    return lines[0:1] + lines[1:2] + lines[2:3]


def last_kernel(bounds, entries, *refs):
    blocks, (fa, fb, ga, gb, ha, hb), state, (kept, given) = refs[:8], refs[8:14], refs[14:20], refs[20:22]
    m, s, p, mb, sb, pb, lse_ref, w_ref, l_ref = refs[22:]
    for ref, value in zip((m, s, p, mb, sb, pb), state):
        ref[...] = value[...]
    for pair in range(PAIRS):
        fill_pair(w_ref, pair, *blocks[2 * pair : 2 * pair + 2])

    def over(pair, _):
        score_tiles(w_ref, pair, ha, 2, l_ref, mb, sb)
        score_tiles(w_ref, pair, hb, 5, l_ref, mb, sb)
        take_rows(pair, 1, bounds, entries, l_ref, pb, False)
        return 0

    lax.fori_loop(0, PAIRS, over, 0)
    score_tiles(w_ref, 3, ga, 0, l_ref, mb, sb)
    score_tiles(w_ref, 3, gb, 3, l_ref, mb, sb)
    take_rows(3, 1, bounds, entries, l_ref, pb, True)
    score_tiles(w_ref, 3, fa, 0, l_ref, m, s)
    score_tiles(w_ref, 3, fb, 3, l_ref, m, s)
    take_rows(3, 0, bounds, entries, l_ref, p)
    for group, (mm, ss, pp) in enumerate(((m, s, p), (mb, sb, pb))):
        for t in range(WINDOWS // 2):
            top = jnp.max(mm[t], 0, keepdims=True)
            total = jnp.sum(ss[t] * jnp.exp(mm[t] - top), 0, keepdims=True)
            value = jnp.broadcast_to(top + jnp.log(total), (8, TILE))
            lse_ref[2 * t] = value[:, :128]
            lse_ref[2 * t + 1] = value[:, 128:]
        for half, out in enumerate((kept, given)):
            for k in range(4):
                rec = half * 4 + k
                shift = 64 * (rec % 2)
                rows = jnp.concatenate([pp[0, rec * 128 : rec * 128 + 128, :], pp[1, rec * 128 : rec * 128 + 128, :]], 1)
                window = rec * 3 // 2
                value = jnp.concatenate([lse_ref[window], lse_ref[window + 1]], 1)
                if shift:
                    rows = pltpu.roll(rows, TILE - shift, 1)
                    value = pltpu.roll(value, TILE - shift, 1)
                out[group * 4 + k, 0:128, :] = rows.astype(jnp.bfloat16)
                out[group * 4 + k, 128:144, :] = split_parts(value)


def join_kernel(where, mine, theirs, *outs):
    place = where[0]
    for group in range(2):
        for step in range(4):
            rec = group * 4 + (place + step) % 4
            out = outs[group * 4 + step]
            one, two = mine[rec], theirs[rec]
            picked = one[0:128].astype(jnp.float32) + two[0:128].astype(jnp.float32)
            out[0:128, :] = picked.astype(jnp.bfloat16)
            a, b = joined_parts(one[128:144]), joined_parts(two[128:144])
            top = jnp.maximum(a, b)
            value = top + jnp.log(jnp.exp(a - top) + jnp.exp(b - top))
            out[128:144, :] = split_parts(jnp.broadcast_to(value, (8, TILE)))


DEPTH = 8


def align_kernel(lengths, *refs):
    parts, (logprob, path, turned, scores) = refs[:8], refs[8:]
    frames = logprob.shape[0]
    picked = parts[0][0:128, :].astype(jnp.float32)
    for part in parts[1:]:
        picked = picked + part[0:128, :].astype(jnp.float32)
    norms = []
    for part in parts:
        norms.append(joined_parts(part[128:144, :]))
    top = functools.reduce(jnp.maximum, norms)
    norm = top + jnp.log(sum(jnp.exp(value - top) for value in norms))
    table = (picked - norm).T[:frames]
    logprob[...] = table
    lanes = lax.broadcasted_iota(jnp.int32, (1, 128), 1)
    for d in range(DEPTH):
        turned[d] = table if d == 0 else pltpu.roll(table, d, 1)

    def advance(score, first, count):
        copies = [score] + [jnp.where(lanes < d, negative_fill, pltpu.roll(score, d, 1)) for d in range(1, count + 1)]
        for i in range(count):
            for d in range(count - i):
                emitted = turned[d, pl.ds(first + i, 1), :]
                copies[d] = jnp.maximum(copies[d], copies[d + 1]) + emitted
            scores[pl.ds(first + i, 1), :] = copies[0]
        return copies[0]

    score = jnp.where(lanes == 0, table[0:1], negative_fill)
    scores[0:1, :] = score
    score = advance(score, 1, DEPTH - 1)
    lax.fori_loop(1, frames // DEPTH, lambda b, now: advance(now, pl.multiple_of(b * DEPTH, DEPTH), DEPTH), score)
    final = scores[pl.ds(lengths[0] - 1, 1), :]
    hit = jnp.sum(jnp.where(lanes == lengths[1] - 1, final, 0.0), 1, keepdims=True)
    path[...] = jnp.broadcast_to(hit, path.shape)


def label_entries(labels, vocab_index, z, y, core):
    flat = labels.reshape(-1)
    local = flat % (NZ * NY * 256)
    chip = local // 256
    owner_y = chip % NY
    dz = (chip // NY - z) % NZ
    table = jnp.where(core == 0, jnp.asarray(place_table()[0]), jnp.asarray(place_table()[1]))
    kinds = lax.iota(jnp.int32, 2 * NZ)
    kind = jnp.where(owner_y == y, dz, NZ + dz)
    place = jnp.sum(jnp.where(kind[:, None] == kinds[None], table[None], 0), 1)
    mine = (flat // (NZ * NY * 256) == vocab_index) & ((owner_y == y) | (owner_y == 3 - y))
    place = jnp.where(mine, place, 2 * PAIRS)
    pair = place // 2
    column = place % 2 * 256 + local % 256
    ids = lax.iota(jnp.int32, flat.shape[0])
    sort_key = pair * 1024 + ids
    rank = jnp.sum((sort_key[None, :] < sort_key[:, None]).astype(jnp.int32), 1)
    value = column * 1024 + ids
    entries = jnp.sum(jnp.where(rank[:, None] == ids[None, :], value[:, None], 0), 0)
    steps = lax.iota(jnp.int32, 8)
    bounds = jnp.sum((pair[:, None] < steps[None, :]).astype(jnp.int32), 0)
    return bounds, entries


def body(features, head_weight, labels, audio_len, transcript_len):
    rec_dev, frames, width = features.shape
    rows = rec_dev * frames
    vocab_index = lax.axis_index("vocab")
    rec = lax.axis_index("rec")
    core, y, z = rec % 2, rec // 2 % NY, rec // (2 * NY)

    def send(array, step0, step1=None):
        return lax.ppermute(array, "rec", moves(step0, step1 if step1 is not None else None))

    def both(array, step):
        return send(array, step, step)

    own = head_weight.T
    other = both(own, other_core)
    fa = features.reshape(rows, width)
    fb = both(fa, other_core)
    l1 = both(labels, other_core)
    half_labels = jnp.concatenate([labels, l1])
    l2 = both(half_labels, beside)
    is0 = core == 0
    o0 = jnp.concatenate([jnp.where(is0, own, other), jnp.where(is0, other, own)])
    ga = both(fa[:EARLY], beside)
    op1 = send(o0, up, down)
    op2 = send(o0, None, mirror)
    ha = both(fa[EARLY:], beside)
    op3 = send(op1, up, down)
    op4 = both(op1, mirror)
    op5 = send(op3, up, down)
    op7 = send(op3, mirror)
    op6 = send(jnp.where(is0, op5, op4), up, down)
    gb = both(ga, other_core)
    op8 = send(jnp.where(is0, op7, op6), up, down)
    op9 = send(op6, mirror)
    hb = both(ha, other_core)
    s1 = jnp.where(is0, op7, o0)
    s2 = jnp.where(is0, op9, op2)

    ba, ea = label_entries(half_labels, vocab_index, z, y, core)
    bb, eb = label_entries(l2, vocab_index, z, y, core)
    bounds, entries = jnp.stack([ba, bb]), jnp.stack([ea, eb])

    f32 = jnp.float32
    state = (
        jax.ShapeDtypeStruct((WINDOWS // 2, 8, TILE), f32),
        jax.ShapeDtypeStruct((WINDOWS // 2, 8, TILE), f32),
        jax.ShapeDtypeStruct((2, 8 * 128, 128), f32),
    )
    logits_scratch = pltpu.VMEM((WINDOWS, BLOCK, 128), f32)

    def call(kernel, out_shape, operands, pairs, gflop, extra=(), limit=28):
        return pl.pallas_call(
            kernel,
            out_shape=out_shape,
            in_specs=[SMEM, SMEM, *([VMEM] * len(operands))],
            out_specs=[VMEM] * len(out_shape),
            scratch_shapes=[*extra, pltpu.VMEM((pairs, BLOCK, width), jnp.bfloat16), logits_scratch],
            cost_estimate=pl.CostEstimate(flops=int(gflop * 1e9), bytes_accessed=0, transcendentals=0),
            compiler_params=pltpu.CompilerParams(vmem_limit_bytes=limit * 2**20),
        )(bounds, entries, *operands)

    ma = call(first_kernel, state, (op1, op3, fa, fb), 1, 4)
    ma = call(second_kernel, state, (op4, op5, fa, fb, *ma), 1, 4)
    *ma, mb, sb, pb = call(third_kernel, state + state, (op1, op3, op4, op5, op6, s1, fa, fb, ga, gb, *ma), 3, 9)
    packed = jax.ShapeDtypeStruct((8, 144, TILE), jnp.bfloat16)
    kept, given = call(
        last_kernel,
        (packed, packed),
        (op1, op3, op4, op5, op6, s1, op8, s2, fa, fb, ga, gb, ha, hb, *ma, mb, sb, pb),
        PAIRS,
        9,
        [*(pltpu.VMEM(leaf.shape, leaf.dtype) for leaf in state + state), pltpu.VMEM((WINDOWS, 8, 128), f32)],
    )
    taken = both(given, other_core)
    payload = jax.ShapeDtypeStruct((144, TILE), jnp.bfloat16)
    sent = pl.pallas_call(
        join_kernel,
        out_shape=[payload] * 8,
        in_specs=[SMEM, VMEM, VMEM],
        out_specs=[VMEM] * 8,
        compiler_params=pltpu.CompilerParams(vmem_limit_bytes=8 * 2**20),
    )(vocab_index[None], kept, taken)
    vocabs = lax.axis_size("vocab")
    groups = lax.axis_size("rec")
    got = []
    for side in range(2):
        for step in range(vocabs):
            part = sent[side * 4 + step]
            if side or step:
                pairs = [
                    (g * vocabs + v, (g ^ (2 * side)) * vocabs + (v + step) % vocabs)
                    for g in range(groups)
                    for v in range(vocabs)
                ]
                part = lax.ppermute(part, ("rec", "vocab"), pairs)
            got.append(part)
    log_prob, path = pl.pallas_call(
        align_kernel,
        out_shape=[jax.ShapeDtypeStruct((frames, 128), f32), jax.ShapeDtypeStruct((8, 128), f32)],
        in_specs=[SMEM, *([VMEM] * 8)],
        out_specs=[VMEM] * 2,
        scratch_shapes=[pltpu.VMEM((DEPTH, frames, 128), f32), pltpu.VMEM((frames, 128), f32)],
        compiler_params=pltpu.CompilerParams(vmem_limit_bytes=8 * 2**20),
    )(jnp.concatenate([audio_len, transcript_len]), *got)
    return log_prob[None], path[0, :1]


def solution(mesh):
    placed = (
        P("rec", None, None),
        P(None, ("vocab", "rec")),
        P("rec", None),
        P(("rec", "vocab")),
        P(("rec", "vocab")),
    )

    return jax.shard_map(
        body,
        mesh=mesh,
        in_specs=placed,
        out_specs=(P(("rec", "vocab"), None, None), P(("rec", "vocab"))),
        check_vma=False,
    )
```

```python
import functools

import jax
import jax.numpy as jnp
import numpy as np
from jax import lax
from jax.experimental import pallas as pl
from jax.experimental.pallas import tpu as pltpu
from jax.sharding import PartitionSpec as P


negative_fill = -1e30
NZ, NY = 8, 4
TILE = 256
BLOCK = 512
PAIRS = 4
WINDOWS = 12
EARLY = 512
ANY = pl.BlockSpec(memory_space=pl.ANY)
VMEM = pl.BlockSpec(memory_space=pltpu.VMEM)
SMEM = pl.BlockSpec(memory_space=pltpu.SMEM)
LOWEST = -3.0e38


def rec_index(z, y, core):
    return ((z % NZ) * NY + y % NY) * 2 + core


def moves(step0=None, step1=None):
    pairs = []
    for core, step in ((0, step0), (1, step1)):
        if step is None:
            continue
        for z in range(NZ):
            for y in range(NY):
                pairs.append((rec_index(z, y, core), rec_index(*step(z, y, core))))
    return pairs


def other_core(z, y, core):
    return z, y, 1 - core


def up(z, y, core):
    return z + 1, y, core


def down(z, y, core):
    return z - 1, y, core


def mirror(z, y, core):
    return z, 3 - y, core


def beside(z, y, core):
    return z, y ^ 1, core


def across(z, y, core):
    return z, y ^ 1, 1 - core


def place_table():
    table = np.full((2, 2 * NZ), 2 * PAIRS, np.int32)
    order0 = [(-1, 0), (-2, 0), (-1, 1), (-3, 0), (-4, 0), (-2, 1), (-3, 1), (-4, 1)]
    order1 = [(1, 0), (2, 0), (1, 1), (3, 0), (2, 1), (0, 0), (3, 1), (0, 1)]
    for core, order in ((0, order0), (1, order1)):
        for place, (dz, far) in enumerate(order):
            table[core, far * NZ + dz % NZ] = place
    return table


def score_jobs(w_ref, pair, jobs):
    def multiply(job):
        f_ref, t, at, l_ref = job[:4]
        tile = lax.dot_general(
            w_ref[pair],
            f_ref[t * TILE : (t + 1) * TILE, :],
            (((1,), (1,)), ((), ())),
            preferred_element_type=jnp.float32,
        )
        l_ref[2 * at] = tile[:, :128]
        l_ref[2 * at + 1] = tile[:, 128:]

    def reduce(job):
        at, l_ref, m_ref, s_ref = job[2:]
        for side in range(2):
            lanes = slice(128 * side, 128 * side + 128)
            cube = l_ref[2 * at + side].reshape(BLOCK // 8, 8, 128)
            old = m_ref[at, :, lanes]
            top = jnp.maximum(jnp.max(cube, 0), old)
            s_ref[at, :, lanes] = s_ref[at, :, lanes] * jnp.exp(old - top) + jnp.sum(jnp.exp(cube - top[None]), 0)
            m_ref[at, :, lanes] = top

    multiply(jobs[0])
    for now, later in zip(jobs, jobs[1:]):
        multiply(later)
        reduce(now)
    reduce(jobs[-1])


def jobs_of(parts, l_ref, m_ref, s_ref):
    return [
        (f_ref, t, first + t, l_ref, m_ref, s_ref) for f_ref, first in parts for t in range(f_ref.shape[0] // TILE)
    ]


def take_rows(pair, which, bounds, entries, l_ref, p_ref, early=None):
    def one(k, _):
        entry = entries[which, k]
        row = entry // 1024
        item = entry % 1024
        for side in range(2):
            window = (item // 128) * 3 // 2 + side

            def copy(window=window, side=side):
                p_ref[side, pl.ds(item, 1), :] = l_ref[window, pl.ds(row, 1), :]

            if early is None:
                copy()
            else:
                inside = window % (WINDOWS // 2) < EARLY // 128
                pl.when(inside if early else jnp.logical_not(inside))(copy)
        return 0

    lax.fori_loop(bounds[which, pair], bounds[which, pair + 1], one, 0)


def fill_pair(w_ref, pair, one, two):
    w_ref[pair, 0 : BLOCK // 2] = one[...]
    w_ref[pair, BLOCK // 2 : BLOCK] = two[...]


def first_kernel(bounds, entries, one, two, fa, fb, m, s, p, w_ref, l_ref):
    m[...] = jnp.full_like(m, LOWEST)
    s[...] = jnp.zeros_like(s)
    p[...] = jnp.zeros_like(p)
    fill_pair(w_ref, 0, one, two)
    score_jobs(w_ref, 0, jobs_of(((fa, 0), (fb, 3)), l_ref, m, s))
    take_rows(0, 0, bounds, entries, l_ref, p)


def second_kernel(bounds, entries, one, two, fa, fb, m_in, s_in, p_in, m, s, p, w_ref, l_ref):
    m[...] = m_in[...]
    s[...] = s_in[...]
    p[...] = p_in[...]
    fill_pair(w_ref, 0, one, two)
    score_jobs(w_ref, 0, jobs_of(((fa, 0), (fb, 3)), l_ref, m, s))
    take_rows(1, 0, bounds, entries, l_ref, p)


def third_kernel(bounds, entries, *refs):
    blocks, (fa, fb, ga, gb, m_in, s_in, p_in), (m, s, p, mb, sb, pb, w_ref, l_ref) = refs[:6], refs[6:13], refs[13:]
    m[...] = m_in[...]
    s[...] = s_in[...]
    p[...] = p_in[...]
    mb[...] = jnp.full_like(mb, LOWEST)
    sb[...] = jnp.zeros_like(sb)
    pb[...] = jnp.zeros_like(pb)
    for pair in range(3):
        fill_pair(w_ref, pair, *blocks[2 * pair : 2 * pair + 2])
    score_jobs(w_ref, 2, jobs_of(((fa, 0), (fb, 3)), l_ref, m, s))
    take_rows(2, 0, bounds, entries, l_ref, p)

    def over(pair, _):
        score_jobs(w_ref, pair, jobs_of(((ga, 0), (gb, 3)), l_ref, mb, sb))
        take_rows(pair, 1, bounds, entries, l_ref, pb, True)
        return 0

    lax.fori_loop(0, 3, over, 0)


def split_parts(value):
    high = value.astype(jnp.bfloat16).astype(jnp.float32)
    middle = (value - high).astype(jnp.bfloat16).astype(jnp.float32)
    low = value - high - middle
    line = lax.broadcasted_iota(jnp.int32, value.shape, 0)
    parts = jnp.where(line == 0, high, jnp.where(line == 1, middle, jnp.where(line == 2, low, 0.0)))
    return jnp.concatenate([parts, jnp.zeros_like(parts)], 0).astype(jnp.bfloat16)


def joined_parts(lines):
    lines = lines.astype(jnp.float32)
    return lines[0:1] + lines[1:2] + lines[2:3]


def last_kernel(bounds, entries, *refs):
    blocks, (fa, fb, ga, gb, ha, hb), state, (kept, given) = refs[:8], refs[8:14], refs[14:20], refs[20:22]
    m, s, p, mb, sb, pb, lse_ref, lb_ref, w_ref, l_ref = refs[22:]
    for ref, value in zip((m, s, p, mb, sb, pb), state):
        ref[...] = value[...]
    for pair in range(PAIRS):
        fill_pair(w_ref, pair, *blocks[2 * pair : 2 * pair + 2])

    def over(pair, _):
        score_jobs(w_ref, pair, jobs_of(((ha, 2), (hb, 5)), lb_ref, mb, sb))
        take_rows(pair, 1, bounds, entries, lb_ref, pb, False)
        return 0

    lax.fori_loop(0, PAIRS, over, 0)
    later = jobs_of(((ga, 0), (gb, 3)), lb_ref, mb, sb)
    score_jobs(w_ref, 3, later + jobs_of(((fa, 0), (fb, 3)), l_ref, m, s))
    take_rows(3, 1, bounds, entries, lb_ref, pb, True)
    take_rows(3, 0, bounds, entries, l_ref, p)
    for group, (mm, ss, pp) in enumerate(((m, s, p), (mb, sb, pb))):
        for t in range(WINDOWS // 2):
            top = jnp.max(mm[t], 0, keepdims=True)
            total = jnp.sum(ss[t] * jnp.exp(mm[t] - top), 0, keepdims=True)
            value = jnp.broadcast_to(top + jnp.log(total), (8, TILE))
            lse_ref[2 * t] = value[:, :128]
            lse_ref[2 * t + 1] = value[:, 128:]
        for half, out in enumerate((kept, given)):
            for k in range(4):
                rec = half * 4 + k
                shift = 64 * (rec % 2)
                rows = jnp.concatenate([pp[0, rec * 128 : rec * 128 + 128, :], pp[1, rec * 128 : rec * 128 + 128, :]], 1)
                window = rec * 3 // 2
                value = jnp.concatenate([lse_ref[window], lse_ref[window + 1]], 1)
                if shift:
                    rows = pltpu.roll(rows, TILE - shift, 1)
                    value = pltpu.roll(value, TILE - shift, 1)
                out[group * 4 + k, 0:128, :] = rows.astype(jnp.bfloat16)
                out[group * 4 + k, 128:144, :] = split_parts(value)


def join_kernel(where, mine, theirs, out):
    odd = where[0]
    for group in range(2):
        for k in range(4):
            rec = group * 4 + k
            to = (group ^ odd) * 4 + k
            one, two = mine[rec], theirs[rec]
            picked = one[0:128].astype(jnp.float32) + two[0:128].astype(jnp.float32)
            out[to, 0:128, :] = picked.astype(jnp.bfloat16)
            a, b = joined_parts(one[128:144]), joined_parts(two[128:144])
            top = jnp.maximum(a, b)
            value = top + jnp.log(jnp.exp(a - top) + jnp.exp(b - top))
            out[to, 128:144, :] = split_parts(jnp.broadcast_to(value, (8, TILE)))


DEPTH = 8


def align_kernel(lengths, parts, logprob, path, turned, scores):
    frames = logprob.shape[0]
    picked = parts[0, 0:128, :].astype(jnp.float32)
    for k in range(1, 8):
        picked = picked + parts[k, 0:128, :].astype(jnp.float32)
    norms = [joined_parts(parts[k, 128:144, :]) for k in range(8)]
    top = functools.reduce(jnp.maximum, norms)
    norm = top + jnp.log(sum(jnp.exp(value - top) for value in norms))
    table = (picked - norm).T[:frames]
    logprob[...] = table
    lanes = lax.broadcasted_iota(jnp.int32, (1, 128), 1)
    for d in range(DEPTH):
        turned[d] = table if d == 0 else pltpu.roll(table, d, 1)

    def advance(score, first, count):
        copies = [score] + [jnp.where(lanes < d, negative_fill, pltpu.roll(score, d, 1)) for d in range(1, count + 1)]
        for i in range(count):
            for d in range(count - i):
                emitted = turned[d, pl.ds(first + i, 1), :]
                copies[d] = jnp.maximum(copies[d], copies[d + 1]) + emitted
            scores[pl.ds(first + i, 1), :] = copies[0]
        return copies[0]

    score = jnp.where(lanes == 0, table[0:1], negative_fill)
    scores[0:1, :] = score
    score = advance(score, 1, DEPTH - 1)
    lax.fori_loop(1, frames // DEPTH, lambda b, now: advance(now, pl.multiple_of(b * DEPTH, DEPTH), DEPTH), score)
    final = scores[pl.ds(lengths[0] - 1, 1), :]
    hit = jnp.sum(jnp.where(lanes == lengths[1] - 1, final, 0.0), 1, keepdims=True)
    path[...] = jnp.broadcast_to(hit, path.shape)


def label_entries(labels, vocab_index, z, y, core):
    flat = labels.reshape(-1)
    local = flat % (NZ * NY * 256)
    chip = local // 256
    owner_y = chip % NY
    dz = (chip // NY - z) % NZ
    table = jnp.where(core == 0, jnp.asarray(place_table()[0]), jnp.asarray(place_table()[1]))
    kinds = lax.iota(jnp.int32, 2 * NZ)
    kind = jnp.where(owner_y == y, dz, NZ + dz)
    place = jnp.sum(jnp.where(kind[:, None] == kinds[None], table[None], 0), 1)
    mine = (flat // (NZ * NY * 256) == vocab_index) & ((owner_y == y) | (owner_y == 3 - y))
    place = jnp.where(mine, place, 2 * PAIRS)
    pair = place // 2
    column = place % 2 * 256 + local % 256
    ids = lax.iota(jnp.int32, flat.shape[0])
    sort_key = pair * 1024 + ids
    rank = jnp.sum((sort_key[None, :] < sort_key[:, None]).astype(jnp.int32), 1)
    value = column * 1024 + ids
    entries = jnp.sum(jnp.where(rank[:, None] == ids[None, :], value[:, None], 0), 0)
    steps = lax.iota(jnp.int32, 8)
    bounds = jnp.sum((pair[:, None] < steps[None, :]).astype(jnp.int32), 0)
    return bounds, entries


def body(features, head_weight, labels, audio_len, transcript_len):
    rec_dev, frames, width = features.shape
    rows = rec_dev * frames
    vocab_index = lax.axis_index("vocab")
    rec = lax.axis_index("rec")
    core, y, z = rec % 2, rec // 2 % NY, rec // (2 * NY)

    def send(array, step0, step1=None):
        return lax.ppermute(array, "rec", moves(step0, step1 if step1 is not None else None))

    def both(array, step):
        return send(array, step, step)

    own = head_weight.T
    other = both(own, other_core)
    is0 = core == 0
    o0 = jnp.concatenate([jnp.where(is0, own, other), jnp.where(is0, other, own)])
    op1 = send(o0, up, down)
    op2 = send(o0, None, mirror)
    fa = features.reshape(rows, width)
    fb = both(fa, other_core)
    l1 = both(labels, other_core)
    l2 = both(labels, beside)
    l3 = both(labels, across)
    ga = both(fa[:EARLY], beside)
    ha = both(fa[EARLY:], beside)
    op3 = send(op1, up, down)
    op4 = both(op1, mirror)
    op5 = send(op3, up, down)
    op7 = send(op3, mirror)
    op6 = send(jnp.where(is0, op5, op4), up, down)
    gb = both(ga, other_core)
    op8 = send(jnp.where(is0, op7, op6), up, down)
    op9 = send(op6, mirror)
    hb = both(ha, other_core)
    s1 = jnp.where(is0, op7, o0)
    s2 = jnp.where(is0, op9, op2)

    ba, ea = label_entries(jnp.concatenate([labels, l1]), vocab_index, z, y, core)
    bb, eb = label_entries(jnp.concatenate([l2, l3]), vocab_index, z, y, core)
    bounds, entries = jnp.stack([ba, bb]), jnp.stack([ea, eb])

    f32 = jnp.float32
    state = (
        jax.ShapeDtypeStruct((WINDOWS // 2, 8, TILE), f32),
        jax.ShapeDtypeStruct((WINDOWS // 2, 8, TILE), f32),
        jax.ShapeDtypeStruct((2, 8 * 128, 128), f32),
    )
    logits_scratch = pltpu.VMEM((WINDOWS, BLOCK, 128), f32)

    def call(kernel, out_shape, operands, pairs, gflop, limit, extra=()):
        return pl.pallas_call(
            kernel,
            out_shape=out_shape,
            in_specs=[SMEM, SMEM, *([VMEM] * len(operands))],
            out_specs=[VMEM] * len(out_shape),
            scratch_shapes=[*extra, pltpu.VMEM((pairs, BLOCK, width), jnp.bfloat16), logits_scratch],
            cost_estimate=pl.CostEstimate(flops=int(gflop * 1e9), bytes_accessed=0, transcendentals=0),
            compiler_params=pltpu.CompilerParams(vmem_limit_bytes=limit * 2**20),
        )(bounds, entries, *operands)

    ma = call(first_kernel, state, (op1, op3, fa, fb), 1, 4, 14)
    ma = call(second_kernel, state, (op4, op5, fa, fb, *ma), 1, 4, 14)
    *ma, mb, sb, pb = call(third_kernel, state + state, (op1, op3, op4, op5, op6, s1, fa, fb, ga, gb, *ma), 3, 9, 18)
    packed = jax.ShapeDtypeStruct((8, 144, TILE), jnp.bfloat16)
    kept, given = call(
        last_kernel,
        (packed, packed),
        (op1, op3, op4, op5, op6, s1, op8, s2, fa, fb, ga, gb, ha, hb, *ma, mb, sb, pb),
        PAIRS,
        9,
        24,
        [*(pltpu.VMEM(leaf.shape, leaf.dtype) for leaf in state + state), pltpu.VMEM((WINDOWS, 8, 128), f32), logits_scratch],
    )
    taken = both(given, other_core)
    sent = pl.pallas_call(
        join_kernel,
        out_shape=packed,
        in_specs=[SMEM, VMEM, VMEM],
        out_specs=VMEM,
        compiler_params=pltpu.CompilerParams(vmem_limit_bytes=8 * 2**20),
    )((y % 2)[None], kept, taken)
    vocabs = lax.axis_size("vocab")
    owners = [
        [rec_index(z, y + side, core) * vocabs + v for side in range(2) for v in range(vocabs)]
        for z in range(NZ)
        for y in range(0, NY, 2)
        for core in range(2)
    ]
    got = lax.all_to_all(sent, ("rec", "vocab"), 0, 0, tiled=True, axis_index_groups=owners)
    log_prob, path = pl.pallas_call(
        align_kernel,
        out_shape=[jax.ShapeDtypeStruct((frames, 128), f32), jax.ShapeDtypeStruct((8, 128), f32)],
        in_specs=[SMEM, VMEM],
        out_specs=[VMEM] * 2,
        scratch_shapes=[pltpu.VMEM((DEPTH, frames, 128), f32), pltpu.VMEM((frames, 128), f32)],
        compiler_params=pltpu.CompilerParams(vmem_limit_bytes=8 * 2**20),
    )(jnp.concatenate([audio_len, transcript_len]), got)
    return log_prob[None], path[0, :1]


def solution(mesh):
    placed = (
        P("rec", None, None),
        P(None, ("vocab", "rec")),
        P("rec", None),
        P(("rec", "vocab")),
        P(("rec", "vocab")),
    )

    return jax.shard_map(
        body,
        mesh=mesh,
        in_specs=placed,
        out_specs=(P(("rec", "vocab"), None, None), P(("rec", "vocab"))),
        check_vma=False,
    )
```

```python
import functools

import jax
import jax.numpy as jnp
import numpy as np
from jax import lax
from jax.experimental import pallas as pl
from jax.experimental.pallas import tpu as pltpu
from jax.sharding import PartitionSpec as P


negative_fill = -1e30
NZ, NY = 8, 4
TILE = 256
BLOCK = 512
PAIRS = 4
WINDOWS = 12
EARLY = 512
ANY = pl.BlockSpec(memory_space=pl.ANY)
VMEM = pl.BlockSpec(memory_space=pltpu.VMEM)
SMEM = pl.BlockSpec(memory_space=pltpu.SMEM)
LOWEST = -3.0e38


def rec_index(z, y, core):
    return ((z % NZ) * NY + y % NY) * 2 + core


def moves(step0=None, step1=None):
    pairs = []
    for core, step in ((0, step0), (1, step1)):
        if step is None:
            continue
        for z in range(NZ):
            for y in range(NY):
                pairs.append((rec_index(z, y, core), rec_index(*step(z, y, core))))
    return pairs


def other_core(z, y, core):
    return z, y, 1 - core


def up(z, y, core):
    return z + 1, y, core


def down(z, y, core):
    return z - 1, y, core


def mirror(z, y, core):
    return z, 3 - y, core


def beside(z, y, core):
    return z, y ^ 1, core


def across(z, y, core):
    return z, y ^ 1, 1 - core


def place_table():
    table = np.full((2, 2 * NZ), 2 * PAIRS, np.int32)
    order0 = [(-1, 0), (-2, 0), (-1, 1), (-3, 0), (-4, 0), (-2, 1), (-3, 1), (-4, 1)]
    order1 = [(1, 0), (2, 0), (1, 1), (3, 0), (2, 1), (0, 0), (3, 1), (0, 1)]
    for core, order in ((0, order0), (1, order1)):
        for place, (dz, far) in enumerate(order):
            table[core, far * NZ + dz % NZ] = place
    return table


def score_jobs(jobs):
    def multiply(w, f_ref, t, l_ref, window, *_):
        tile = lax.dot_general(
            w[...], f_ref[t * TILE : (t + 1) * TILE, :], (((1,), (1,)), ((), ())), preferred_element_type=jnp.float32
        )
        l_ref[window] = tile[:, :128]
        l_ref[window + 1] = tile[:, 128:]

    def reduce(w, f_ref, t, l_ref, window, m_ref, s_ref, at):
        for side in range(2):
            lanes = slice(128 * side, 128 * side + 128)
            cube = l_ref[window + side].reshape(w.shape[0] // 8, 8, 128)
            old = m_ref[at, :, lanes]
            top = jnp.maximum(jnp.max(cube, 0), old)
            s_ref[at, :, lanes] = s_ref[at, :, lanes] * jnp.exp(old - top) + jnp.sum(jnp.exp(cube - top[None]), 0)
            m_ref[at, :, lanes] = top

    multiply(*jobs[0])
    for now, later in zip(jobs, jobs[1:]):
        multiply(*later)
        reduce(*now)
    reduce(*jobs[-1])


def jobs_of(w, parts, l_ref, m_ref, s_ref):
    jobs = []
    for f_ref, first in parts:
        for t in range(f_ref.shape[0] // TILE):
            jobs.append((w, f_ref, t, l_ref, 2 * len(jobs), m_ref, s_ref, first + t))
    return jobs


GROUP = 8


def take_rows(first, last, which, bounds, entries, l_ref, p_ref, early=None):
    low, high = bounds[which, first], bounds[which, last]

    def group(g, _):
        found = []
        for j in range(GROUP):
            entry = entries[which, jnp.minimum(low + g * GROUP + j, high - 1)]
            column = (entry >> 10) - first * BLOCK
            item = entry & 1023
            for side in range(2):
                window = (((item >> 7) * 3) >> 1) + side
                to = item
                if early is not None:
                    within = jnp.where(window >= 6, window - 6, window)
                    far = window >= 6
                    if early:
                        inside = within < EARLY // 128
                        window = jnp.where(far, window - 2, window)
                    else:
                        inside = within >= EARLY // 128
                        window = jnp.where(far, window - 8, window - 4)
                    window = jnp.where(inside, window, 0)
                    to = jnp.where(inside, item, 1024 + j)
                found.append((side, to, l_ref[window, pl.ds(column, 1), :]))
        for side, to, row in found:
            p_ref[side, pl.ds(to, 1), :] = row
        return 0

    lax.fori_loop(0, (high - low + GROUP - 1) >> 3, group, 0)


def fill_columns(w_ref, blocks):
    for k, block in enumerate(blocks):
        w_ref[k * (BLOCK // 2) : (k + 1) * (BLOCK // 2)] = block[...]


def first_kernel(bounds, entries, one, two, fa, fb, m, s, p, w_ref, l_ref):
    m[...] = jnp.full_like(m, LOWEST)
    s[...] = jnp.zeros_like(s)
    p[...] = jnp.zeros_like(p)
    fill_columns(w_ref, (one, two))
    score_jobs(jobs_of(w_ref, ((fa, 0), (fb, 3)), l_ref, m, s))
    take_rows(0, 1, 0, bounds, entries, l_ref, p)


def second_kernel(bounds, entries, one, two, fa, fb, m_in, s_in, p_in, m, s, p, w_ref, l_ref):
    m[...] = m_in[...]
    s[...] = s_in[...]
    p[...] = p_in[...]
    fill_columns(w_ref, (one, two))
    score_jobs(jobs_of(w_ref, ((fa, 0), (fb, 3)), l_ref, m, s))
    take_rows(1, 2, 0, bounds, entries, l_ref, p)


def third_kernel(bounds, entries, *refs):
    blocks, (fa, fb, ga, gb, m_in, s_in, p_in), refs = refs[:6], refs[6:13], refs[13:]
    m, s, p, mb, sb, pb, lb_ref, w_ref, l_ref = refs
    m[...] = m_in[...]
    s[...] = s_in[...]
    p[...] = p_in[...]
    mb[...] = jnp.full_like(mb, LOWEST)
    sb[...] = jnp.zeros_like(sb)
    pb[...] = jnp.zeros_like(pb)
    fill_columns(w_ref, blocks)
    near = jobs_of(w_ref.at[2 * BLOCK : 3 * BLOCK], ((fa, 0), (fb, 3)), l_ref, m, s)
    score_jobs(near + jobs_of(w_ref, ((ga, 0), (gb, 3)), lb_ref, mb, sb))
    take_rows(2, 3, 0, bounds, entries, l_ref, p)
    take_rows(0, 3, 1, bounds, entries, lb_ref, pb, True)


def split_parts(value):
    high = value.astype(jnp.bfloat16).astype(jnp.float32)
    middle = (value - high).astype(jnp.bfloat16).astype(jnp.float32)
    low = value - high - middle
    line = lax.broadcasted_iota(jnp.int32, value.shape, 0)
    parts = jnp.where(line == 0, high, jnp.where(line == 1, middle, jnp.where(line == 2, low, 0.0)))
    return jnp.concatenate([parts, jnp.zeros_like(parts)], 0).astype(jnp.bfloat16)


def joined_parts(lines):
    lines = lines.astype(jnp.float32)
    return lines[0:1] + lines[1:2] + lines[2:3]


def last_kernel(bounds, entries, *refs):
    blocks, (fa, fb, ga, gb, ha, hb), state, (kept, given) = refs[:8], refs[8:14], refs[14:20], refs[20:22]
    m, s, p, mb, sb, pb, lse_ref, lb_ref, lc_ref, w_ref, l_ref = refs[22:]
    for ref, value in zip((m, s, p, mb, sb, pb), state):
        ref[...] = value[...]
    fill_columns(w_ref, blocks)
    final = w_ref.at[3 * BLOCK : 4 * BLOCK]
    jobs = jobs_of(w_ref, ((ha, 2), (hb, 5)), lc_ref, mb, sb)
    jobs += jobs_of(final, ((ga, 0), (gb, 3)), lb_ref, mb, sb)
    score_jobs(jobs + jobs_of(final, ((fa, 0), (fb, 3)), l_ref, m, s))
    take_rows(0, 4, 1, bounds, entries, lc_ref, pb, False)
    take_rows(3, 4, 1, bounds, entries, lb_ref, pb, True)
    take_rows(3, 4, 0, bounds, entries, l_ref, p)
    for group, (mm, ss, pp) in enumerate(((m, s, p), (mb, sb, pb))):
        for t in range(WINDOWS // 2):
            top = jnp.max(mm[t], 0, keepdims=True)
            total = jnp.sum(ss[t] * jnp.exp(mm[t] - top), 0, keepdims=True)
            value = jnp.broadcast_to(top + jnp.log(total), (8, TILE))
            lse_ref[2 * t] = value[:, :128]
            lse_ref[2 * t + 1] = value[:, 128:]
        for half, out in enumerate((kept, given)):
            for k in range(4):
                rec = half * 4 + k
                shift = 64 * (rec % 2)
                rows = jnp.concatenate([pp[0, rec * 128 : rec * 128 + 128, :], pp[1, rec * 128 : rec * 128 + 128, :]], 1)
                window = rec * 3 // 2
                value = jnp.concatenate([lse_ref[window], lse_ref[window + 1]], 1)
                if shift:
                    rows = pltpu.roll(rows, TILE - shift, 1)
                    value = pltpu.roll(value, TILE - shift, 1)
                out[group * 4 + k, 0:128, :] = rows.astype(jnp.bfloat16)
                out[group * 4 + k, 128:144, :] = split_parts(value)


def join_kernel(where, mine, theirs, out):
    odd = where[0]
    early_lanes = lax.broadcasted_iota(jnp.int32, (64, 128), 1) < 64
    for group in range(2):
        for k in range(4):
            rec = group * 4 + k
            to = (group ^ odd) * 4 + k
            one, two = mine[rec], theirs[rec]
            picked = one[0:128].astype(jnp.float32) + two[0:128].astype(jnp.float32)
            out[to, 0:128, :] = picked[:, 0:128].astype(jnp.bfloat16)
            tail = picked[:, 128:256]
            tail = jnp.where(early_lanes, tail[0:64], pltpu.roll(tail[64:128], 64, 1))
            out[to, 128:192, :] = tail.astype(jnp.bfloat16)
            a, b = joined_parts(one[128:144]), joined_parts(two[128:144])
            top = jnp.maximum(a, b)
            value = top + jnp.log(jnp.exp(a - top) + jnp.exp(b - top))
            for side in range(2):
                lanes = jnp.broadcast_to(value[:, 128 * side : 128 * side + 128], (8, 128))
                out[to, 192 + 16 * side : 208 + 16 * side, :] = split_parts(lanes)


DEPTH = 8


def align_kernel(lengths, parts, logprob, path, turned, scores):
    frames = logprob.shape[0]
    picked = parts[0, 0:192, :].astype(jnp.float32)
    for k in range(1, 8):
        picked = picked + parts[k, 0:192, :].astype(jnp.float32)
    sides = []
    for side in range(2):
        rows = slice(192 + 16 * side, 208 + 16 * side)
        norms = [joined_parts(parts[k, rows, :]) for k in range(8)]
        top = functools.reduce(jnp.maximum, norms)
        sides.append(top + jnp.log(sum(jnp.exp(value - top) for value in norms)))
    tail = jnp.concatenate([picked[128:192], pltpu.roll(picked[128:192], 64, 1)], 0) - sides[1]
    table = jnp.concatenate([(picked[0:128] - sides[0]).T, tail.T[0:64]], 0)
    logprob[...] = table
    lanes = lax.broadcasted_iota(jnp.int32, (1, 128), 1)
    for d in range(DEPTH):
        turned[d] = table if d == 0 else pltpu.roll(table, d, 1)

    def advance(score, first, count):
        copies = [score] + [jnp.where(lanes < d, negative_fill, pltpu.roll(score, d, 1)) for d in range(1, count + 1)]
        for i in range(count):
            for d in range(count - i):
                emitted = turned[d, pl.ds(first + i, 1), :]
                copies[d] = jnp.maximum(copies[d], copies[d + 1]) + emitted
            scores[pl.ds(first + i, 1), :] = copies[0]
        return copies[0]

    score = jnp.where(lanes == 0, table[0:1], negative_fill)
    scores[0:1, :] = score
    score = advance(score, 1, DEPTH - 1)
    lax.fori_loop(1, frames // DEPTH, lambda b, now: advance(now, pl.multiple_of(b * DEPTH, DEPTH), DEPTH), score)
    final = scores[pl.ds(lengths[0] - 1, 1), :]
    hit = jnp.sum(jnp.where(lanes == lengths[1] - 1, final, 0.0), 1, keepdims=True)
    path[...] = jnp.broadcast_to(hit, path.shape)


def label_entries(labels, vocab_index, z, y, core):
    flat = labels.reshape(-1)
    local = flat % (NZ * NY * 256)
    chip = local // 256
    owner_y = chip % NY
    dz = (chip // NY - z) % NZ
    table = jnp.where(core == 0, jnp.asarray(place_table()[0]), jnp.asarray(place_table()[1]))
    kinds = lax.iota(jnp.int32, 2 * NZ)
    kind = jnp.where(owner_y == y, dz, NZ + dz)
    place = jnp.sum(jnp.where(kind[:, None] == kinds[None], table[None], 0), 1)
    mine = (flat // (NZ * NY * 256) == vocab_index) & ((owner_y == y) | (owner_y == 3 - y))
    place = jnp.where(mine, place, 2 * PAIRS)
    pair = place // 2
    column = place * 256 + (local // 128 % 2 ^ core) * 128 + local % 128
    ids = lax.iota(jnp.int32, flat.shape[0])
    sort_key = pair * 1024 + ids
    rank = jnp.sum((sort_key[None, :] < sort_key[:, None]).astype(jnp.int32), 1)
    value = column * 1024 + ids
    entries = jnp.sum(jnp.where(rank[:, None] == ids[None, :], value[:, None], 0), 0)
    steps = lax.iota(jnp.int32, 8)
    bounds = jnp.sum((pair[:, None] < steps[None, :]).astype(jnp.int32), 0)
    return bounds, entries


def body(features, head_weight, labels, audio_len, transcript_len):
    rec_dev, frames, width = features.shape
    rows = rec_dev * frames
    vocab_index = lax.axis_index("vocab")
    rec = lax.axis_index("rec")
    core, y, z = rec % 2, rec // 2 % NY, rec // (2 * NY)

    def send(array, step0, step1=None):
        return lax.ppermute(array, "rec", moves(step0, step1 if step1 is not None else None))

    def both(array, step):
        return send(array, step, step)

    own = head_weight.T
    other = both(own, other_core)
    is0 = core == 0
    o0 = jnp.concatenate([own, other])
    op1 = send(o0, up, down)
    op2 = send(o0, None, mirror)
    fa = features.reshape(rows, width)
    fb = both(fa, other_core)
    l1 = both(labels, other_core)
    l2 = both(labels, beside)
    l3 = both(labels, across)
    ga = both(fa[:EARLY], beside)
    ha = both(fa[EARLY:], beside)
    op3 = send(op1, up, down)
    op4 = both(op1, mirror)
    op5 = send(op3, up, down)
    op7 = send(op3, mirror)
    op6 = send(jnp.where(is0, op5, op4), up, down)
    gb = both(ga, other_core)
    op8 = send(jnp.where(is0, op7, op6), up, down)
    op9 = send(op6, mirror)
    hb = both(ha, other_core)
    s1 = jnp.where(is0, op7, o0)
    s2 = jnp.where(is0, op9, op2)

    ba, ea = label_entries(jnp.concatenate([labels, l1]), vocab_index, z, y, core)
    bb, eb = label_entries(jnp.concatenate([l2, l3]), vocab_index, z, y, core)
    bounds = jnp.stack([ba, bb])
    entries = jnp.stack([ea, eb])

    f32 = jnp.float32
    state = (
        jax.ShapeDtypeStruct((WINDOWS // 2, 8, TILE), f32),
        jax.ShapeDtypeStruct((WINDOWS // 2, 8, TILE), f32),
        jax.ShapeDtypeStruct((2, 8 * 128 + GROUP, 128), f32),
    )
    logits_scratch = pltpu.VMEM((WINDOWS, BLOCK, 128), f32)

    def call(kernel, out_shape, operands, pairs, gflop, limit, extra=()):
        return pl.pallas_call(
            kernel,
            out_shape=out_shape,
            in_specs=[SMEM, SMEM, *([VMEM] * len(operands))],
            out_specs=[VMEM] * len(out_shape),
            scratch_shapes=[*extra, pltpu.VMEM((pairs * BLOCK, width), jnp.bfloat16), logits_scratch],
            cost_estimate=pl.CostEstimate(flops=int(gflop * 1e9), bytes_accessed=0, transcendentals=0),
            compiler_params=pltpu.CompilerParams(vmem_limit_bytes=limit * 2**20),
        )(bounds, entries, *operands)

    ma = call(first_kernel, state, (op1, op3, fa, fb), 1, 4, 8)
    ma = call(second_kernel, state, (op4, op5, fa, fb, *ma), 1, 4, 8)
    *ma, mb, sb, pb = call(
        third_kernel,
        state + state,
        (op1, op3, op4, op5, op6, s1, fa, fb, ga, gb, *ma),
        3,
        9,
        17,
        [pltpu.VMEM((2 * EARLY // 128, 3 * BLOCK, 128), f32)],
    )
    packed = jax.ShapeDtypeStruct((8, 144, TILE), jnp.bfloat16)
    kept, given = call(
        last_kernel,
        (packed, packed),
        (op1, op3, op4, op5, op6, s1, op8, s2, fa, fb, ga, gb, ha, hb, *ma, mb, sb, pb),
        PAIRS,
        9,
        20,
        [*(pltpu.VMEM(leaf.shape, leaf.dtype) for leaf in state + state), pltpu.VMEM((WINDOWS, 8, 128), f32),
         pltpu.VMEM((2 * EARLY // 128, BLOCK, 128), f32),
         pltpu.VMEM((WINDOWS - 2 * EARLY // 128, 4 * BLOCK, 128), f32)],
    )
    taken = both(given, other_core)
    sent = pl.pallas_call(
        join_kernel,
        out_shape=jax.ShapeDtypeStruct((8, 224, 128), jnp.bfloat16),
        in_specs=[SMEM, VMEM, VMEM],
        out_specs=VMEM,
        compiler_params=pltpu.CompilerParams(vmem_limit_bytes=8 * 2**20),
    )((y % 2)[None], kept, taken)
    vocabs = lax.axis_size("vocab")
    owners = [
        [rec_index(z, y + side, core) * vocabs + v for side in range(2) for v in range(vocabs)]
        for z in range(NZ)
        for y in range(0, NY, 2)
        for core in range(2)
    ]
    got = lax.all_to_all(sent, ("rec", "vocab"), 0, 0, tiled=True, axis_index_groups=owners)
    log_prob, path = pl.pallas_call(
        align_kernel,
        out_shape=[jax.ShapeDtypeStruct((frames, 128), f32), jax.ShapeDtypeStruct((8, 128), f32)],
        in_specs=[SMEM, VMEM],
        out_specs=[VMEM] * 2,
        scratch_shapes=[pltpu.VMEM((DEPTH, frames, 128), f32), pltpu.VMEM((frames, 128), f32)],
        compiler_params=pltpu.CompilerParams(vmem_limit_bytes=8 * 2**20),
    )(jnp.concatenate([audio_len, transcript_len]), got)
    return log_prob[None], path[0, :1]


def solution(mesh):
    placed = (
        P("rec", None, None),
        P(None, ("vocab", "rec")),
        P("rec", None),
        P(("rec", "vocab")),
        P(("rec", "vocab")),
    )

    return jax.shard_map(
        body,
        mesh=mesh,
        in_specs=placed,
        out_specs=(P(("rec", "vocab"), None, None), P(("rec", "vocab"))),
        check_vma=False,
    )
```

```python
import functools

import jax
import jax.numpy as jnp
import numpy as np
from jax import lax
from jax.experimental import pallas as pl
from jax.experimental.pallas import tpu as pltpu
from jax.sharding import PartitionSpec as P


negative_fill = -1e30
NZ, NY = 8, 4
TILE = 256
BLOCK = 512
PAIRS = 4
WINDOWS = 12
EARLY = 512
ANY = pl.BlockSpec(memory_space=pl.ANY)
VMEM = pl.BlockSpec(memory_space=pltpu.VMEM)
SMEM = pl.BlockSpec(memory_space=pltpu.SMEM)
LOWEST = -3.0e38


def rec_index(z, y, core):
    return ((z % NZ) * NY + y % NY) * 2 + core


def moves(step0=None, step1=None):
    pairs = []
    for core, step in ((0, step0), (1, step1)):
        if step is None:
            continue
        for z in range(NZ):
            for y in range(NY):
                pairs.append((rec_index(z, y, core), rec_index(*step(z, y, core))))
    return pairs


def other_core(z, y, core):
    return z, y, 1 - core


def up(z, y, core):
    return z + 1, y, core


def down(z, y, core):
    return z - 1, y, core


def mirror(z, y, core):
    return z, 3 - y, core


def beside(z, y, core):
    return z, y ^ 1, core


def across(z, y, core):
    return z, y ^ 1, 1 - core


def place_table():
    table = np.full((2, 2 * NZ), 2 * PAIRS, np.int32)
    order0 = [(-1, 0), (-2, 0), (-1, 1), (-3, 0), (-4, 0), (-2, 1), (-3, 1), (-4, 1)]
    order1 = [(1, 0), (2, 0), (1, 1), (3, 0), (2, 1), (0, 0), (3, 1), (0, 1)]
    for core, order in ((0, order0), (1, order1)):
        for place, (dz, far) in enumerate(order):
            table[core, far * NZ + dz % NZ] = place
    return table


def score_jobs(jobs):
    def multiply(w, f_ref, t, l_ref, window, *_):
        tile = lax.dot_general(
            w[...], f_ref[t * TILE : (t + 1) * TILE, :], (((1,), (1,)), ((), ())), preferred_element_type=jnp.float32
        )
        l_ref[window] = tile[:, :128]
        l_ref[window + 1] = tile[:, 128:]

    def reduce(w, f_ref, t, l_ref, window, m_ref, s_ref, at):
        for side in range(2):
            lanes = slice(128 * side, 128 * side + 128)
            cube = l_ref[window + side].reshape(w.shape[0] // 8, 8, 128)
            old = m_ref[at, :, lanes]
            top = jnp.maximum(jnp.max(cube, 0), old)
            s_ref[at, :, lanes] = s_ref[at, :, lanes] * jnp.exp(old - top) + jnp.sum(jnp.exp(cube - top[None]), 0)
            m_ref[at, :, lanes] = top

    multiply(*jobs[0])
    for now, later in zip(jobs, jobs[1:]):
        multiply(*later)
        reduce(*now)
    reduce(*jobs[-1])


def jobs_of(w, parts, l_ref, m_ref, s_ref, packed=False):
    jobs = []
    for f_ref, first in parts:
        for t in range(f_ref.shape[0] // TILE):
            window = 2 * (len(jobs) if packed else first + t)
            jobs.append((w, f_ref, t, l_ref, window, m_ref, s_ref, first + t))
    return jobs


GROUP = 8


def take_rows(first, last, which, bounds, entries, l_ref, p_ref, early=None):
    low, high = bounds[which, first], bounds[which, last]

    def group(g, _):
        found = []
        for j in range(GROUP):
            entry = entries[which, jnp.minimum(low + g * GROUP + j, high - 1)]
            column = (entry >> 10) - first * BLOCK
            item = entry & 1023
            for side in range(2):
                window = (((item >> 7) * 3) >> 1) + side
                to = item
                if early is not None:
                    within = jnp.where(window >= 6, window - 6, window)
                    far = window >= 6
                    if early:
                        inside = within < EARLY // 128
                        window = jnp.where(far, window - 2, window)
                    else:
                        inside = within >= EARLY // 128
                        window = jnp.where(far, window - 8, window - 4)
                    window = jnp.where(inside, window, 0)
                    to = jnp.where(inside, item, 1024 + j)
                found.append((side, to, l_ref[window, pl.ds(column, 1), :]))
        for side, to, row in found:
            p_ref[side, pl.ds(to, 1), :] = row
        return 0

    lax.fori_loop(0, (high - low + GROUP - 1) >> 3, group, 0)


def fill_columns(w_ref, blocks):
    for k, block in enumerate(blocks):
        w_ref[k * (BLOCK // 2) : (k + 1) * (BLOCK // 2)] = block[...]


def prepare_kernel(shard, rows, turned, near, early, late, sems):
    copies = [
        pltpu.make_async_copy(rows, near, sems.at[0]),
        pltpu.make_async_copy(rows.at[0:EARLY], early, sems.at[1]),
        pltpu.make_async_copy(rows.at[EARLY : rows.shape[0]], late, sems.at[2]),
    ]
    for copy in copies:
        copy.start()
    turned[...] = shard[...].T
    for copy in copies:
        copy.wait()


def first_kernel(bounds, entries, one, two, fa, fb, m, s, p, w_ref, l_ref):
    m[...] = jnp.full_like(m, LOWEST)
    s[...] = jnp.zeros_like(s)
    p[...] = jnp.zeros_like(p)
    fill_columns(w_ref, (one, two))
    score_jobs(jobs_of(w_ref, ((fa, 0), (fb, 3)), l_ref, m, s))
    take_rows(0, 1, 0, bounds, entries, l_ref, p)


def second_kernel(bounds, entries, one, two, fa, fb, m_in, s_in, p_in, m, s, p, w_ref, l_ref):
    m[...] = m_in[...]
    s[...] = s_in[...]
    p[...] = p_in[...]
    fill_columns(w_ref, (one, two))
    score_jobs(jobs_of(w_ref, ((fa, 0), (fb, 3)), l_ref, m, s))
    take_rows(1, 2, 0, bounds, entries, l_ref, p)


def beside_kernel(bounds, entries, *refs):
    blocks, (ga, gb), (mb, sb, pb, lb_ref, w_ref, _) = refs[:4], refs[4:6], refs[6:]
    mb[...] = jnp.full_like(mb, LOWEST)
    sb[...] = jnp.zeros_like(sb)
    pb[...] = jnp.zeros_like(pb)
    fill_columns(w_ref, blocks)
    score_jobs(jobs_of(w_ref, ((ga, 0), (gb, 3)), lb_ref, mb, sb, True))
    take_rows(0, 2, 1, bounds, entries, lb_ref, pb, True)


def third_kernel(bounds, entries, *refs):
    blocks, (fa, fb, ga, gb, ha, hb), state, state_out, refs = refs[:6], refs[6:12], refs[12:18], refs[18:24], refs[24:]
    lb_ref, lc_ref, w_ref, l_ref = refs
    for ref, value in zip(state_out, state):
        ref[...] = value[...]
    m, s, p, mb, sb, pb = state_out
    fill_columns(w_ref, blocks)
    newest = w_ref.at[2 * BLOCK : 3 * BLOCK]
    jobs = jobs_of(newest, ((fa, 0), (fb, 3)), l_ref, m, s)
    jobs += jobs_of(newest, ((ga, 0), (gb, 3)), lb_ref, mb, sb, True)
    score_jobs(jobs + jobs_of(w_ref, ((ha, 2), (hb, 5)), lc_ref, mb, sb, True))
    take_rows(2, 3, 0, bounds, entries, l_ref, p)
    take_rows(2, 3, 1, bounds, entries, lb_ref, pb, True)
    take_rows(0, 3, 1, bounds, entries, lc_ref, pb, False)


def split_parts(value):
    high = value.astype(jnp.bfloat16).astype(jnp.float32)
    middle = (value - high).astype(jnp.bfloat16).astype(jnp.float32)
    low = value - high - middle
    line = lax.broadcasted_iota(jnp.int32, value.shape, 0)
    parts = jnp.where(line == 0, high, jnp.where(line == 1, middle, jnp.where(line == 2, low, 0.0)))
    return jnp.concatenate([parts, jnp.zeros_like(parts)], 0).astype(jnp.bfloat16)


def joined_parts(lines):
    lines = lines.astype(jnp.float32)
    return lines[0:1] + lines[1:2] + lines[2:3]


def last_kernel(bounds, entries, *refs):
    blocks, (fa, fb, ga, gb, ha, hb), state, (kept, given) = refs[:2], refs[2:8], refs[8:14], refs[14:16]
    m, s, p, mb, sb, pb, lse_ref, lb_ref, w_ref, l_ref = refs[16:]
    for ref, value in zip((m, s, p, mb, sb, pb), state):
        ref[...] = value[...]
    fill_columns(w_ref, blocks)
    jobs = jobs_of(w_ref, ((fa, 0), (fb, 3)), l_ref, m, s)
    score_jobs(jobs + jobs_of(w_ref, ((ga, 0), (ha, 2), (gb, 3), (hb, 5)), lb_ref, mb, sb))
    take_rows(3, 4, 0, bounds, entries, l_ref, p)
    take_rows(3, 4, 1, bounds, entries, lb_ref, pb)
    for group, (mm, ss, pp) in enumerate(((m, s, p), (mb, sb, pb))):
        for t in range(WINDOWS // 2):
            top = jnp.max(mm[t], 0, keepdims=True)
            total = jnp.sum(ss[t] * jnp.exp(mm[t] - top), 0, keepdims=True)
            value = jnp.broadcast_to(top + jnp.log(total), (8, TILE))
            lse_ref[2 * t] = value[:, :128]
            lse_ref[2 * t + 1] = value[:, 128:]
        for half, out in enumerate((kept, given)):
            for k in range(4):
                rec = half * 4 + k
                shift = 64 * (rec % 2)
                rows = jnp.concatenate([pp[0, rec * 128 : rec * 128 + 128, :], pp[1, rec * 128 : rec * 128 + 128, :]], 1)
                window = rec * 3 // 2
                value = jnp.concatenate([lse_ref[window], lse_ref[window + 1]], 1)
                if shift:
                    rows = pltpu.roll(rows, TILE - shift, 1)
                    value = pltpu.roll(value, TILE - shift, 1)
                out[group * 4 + k, 0:128, :] = rows.astype(jnp.bfloat16)
                out[group * 4 + k, 128:144, :] = split_parts(value)


def join_kernel(where, mine, theirs, out):
    odd = where[0]
    early_lanes = lax.broadcasted_iota(jnp.int32, (64, 128), 1) < 64
    for group in range(2):
        for k in range(4):
            rec = group * 4 + k
            to = (group ^ odd) * 4 + k
            one, two = mine[rec], theirs[rec]
            picked = one[0:128].astype(jnp.float32) + two[0:128].astype(jnp.float32)
            out[to, 0:128, :] = picked[:, 0:128].astype(jnp.bfloat16)
            tail = picked[:, 128:256]
            tail = jnp.where(early_lanes, tail[0:64], pltpu.roll(tail[64:128], 64, 1))
            out[to, 128:192, :] = tail.astype(jnp.bfloat16)
            a, b = joined_parts(one[128:144]), joined_parts(two[128:144])
            top = jnp.maximum(a, b)
            value = top + jnp.log(jnp.exp(a - top) + jnp.exp(b - top))
            for side in range(2):
                lanes = jnp.broadcast_to(value[:, 128 * side : 128 * side + 128], (8, 128))
                out[to, 192 + 16 * side : 208 + 16 * side, :] = split_parts(lanes)


DEPTH = 8


def align_kernel(lengths, parts, logprob, path, turned, scores):
    frames = logprob.shape[0]
    picked = parts[0, 0:192, :].astype(jnp.float32)
    for k in range(1, 8):
        picked = picked + parts[k, 0:192, :].astype(jnp.float32)
    sides = []
    for side in range(2):
        rows = slice(192 + 16 * side, 208 + 16 * side)
        norms = [joined_parts(parts[k, rows, :]) for k in range(8)]
        top = functools.reduce(jnp.maximum, norms)
        sides.append(top + jnp.log(sum(jnp.exp(value - top) for value in norms)))
    tail = jnp.concatenate([picked[128:192], pltpu.roll(picked[128:192], 64, 1)], 0) - sides[1]
    table = jnp.concatenate([(picked[0:128] - sides[0]).T, tail.T[0:64]], 0)
    logprob[...] = table
    lanes = lax.broadcasted_iota(jnp.int32, (1, 128), 1)
    for d in range(DEPTH):
        turned[d] = table if d == 0 else pltpu.roll(table, d, 1)

    def advance(score, first, count):
        copies = [score] + [jnp.where(lanes < d, negative_fill, pltpu.roll(score, d, 1)) for d in range(1, count + 1)]
        for i in range(count):
            for d in range(count - i):
                emitted = turned[d, pl.ds(first + i, 1), :]
                copies[d] = jnp.maximum(copies[d], copies[d + 1]) + emitted
            scores[pl.ds(first + i, 1), :] = copies[0]
        return copies[0]

    score = jnp.where(lanes == 0, table[0:1], negative_fill)
    scores[0:1, :] = score
    score = advance(score, 1, DEPTH - 1)
    lax.fori_loop(1, frames // DEPTH, lambda b, now: advance(now, pl.multiple_of(b * DEPTH, DEPTH), DEPTH), score)
    final = scores[pl.ds(lengths[0] - 1, 1), :]
    path[0] = jnp.sum(jnp.where(lanes == lengths[1] - 1, final, 0.0))


def label_entries(labels, vocab_index, z, y, core):
    flat = labels.reshape(-1)
    local = flat % (NZ * NY * 256)
    chip = local // 256
    owner_y = chip % NY
    dz = (chip // NY - z) % NZ
    table = jnp.where(core == 0, jnp.asarray(place_table()[0]), jnp.asarray(place_table()[1]))
    kinds = lax.iota(jnp.int32, 2 * NZ)
    kind = jnp.where(owner_y == y, dz, NZ + dz)
    place = jnp.sum(jnp.where(kind[:, None] == kinds[None], table[None], 0), 1)
    mine = (flat // (NZ * NY * 256) == vocab_index) & ((owner_y == y) | (owner_y == 3 - y))
    place = jnp.where(mine, place, 2 * PAIRS)
    pair = place // 2
    column = place * 256 + (local // 128 % 2 ^ core) * 128 + local % 128
    ids = lax.iota(jnp.int32, flat.shape[0])
    sort_key = pair * 1024 + ids
    rank = jnp.sum((sort_key[None, :] < sort_key[:, None]).astype(jnp.int32), 1)
    value = column * 1024 + ids
    entries = jnp.sum(jnp.where(rank[:, None] == ids[None, :], value[:, None], 0), 0)
    steps = lax.iota(jnp.int32, 8)
    bounds = jnp.sum((pair[:, None] < steps[None, :]).astype(jnp.int32), 0)
    return bounds, entries


def body(features, head_weight, labels, audio_len, transcript_len):
    rec_dev, frames, width = features.shape
    rows = rec_dev * frames
    vocab_index = lax.axis_index("vocab")
    rec = lax.axis_index("rec")
    core, y, z = rec % 2, rec // 2 % NY, rec // (2 * NY)

    def send(array, step0, step1=None):
        return lax.ppermute(array, "rec", moves(step0, step1 if step1 is not None else None))

    def both(array, step):
        return send(array, step, step)

    columns = head_weight.shape[1]
    own, fa, early, late = pl.pallas_call(
        prepare_kernel,
        out_shape=[
            jax.ShapeDtypeStruct(shape, jnp.bfloat16)
            for shape in ((columns, width), (rows, width), (EARLY, width), (rows - EARLY, width))
        ],
        in_specs=[VMEM, ANY],
        out_specs=[VMEM] * 4,
        scratch_shapes=[pltpu.SemaphoreType.DMA((3,))],
        compiler_params=pltpu.CompilerParams(vmem_limit_bytes=8 * 2**20),
    )(head_weight, features.reshape(rows, width))
    other = both(own, other_core)
    is0 = core == 0
    o0 = jnp.concatenate([own, other])
    op1 = send(o0, up, down)
    op2 = send(o0, None, mirror)
    fb = both(fa, other_core)
    l1 = both(labels, other_core)
    l2 = both(labels, beside)
    l3 = both(labels, across)
    ga = both(early, beside)
    ha = both(late, beside)
    op3 = send(op1, up, down)
    op4 = both(op1, mirror)
    op5 = send(op3, up, down)
    op7 = send(op3, mirror)
    op6 = send(jnp.where(is0, op5, op4), up, down)
    gb = both(ga, other_core)
    op8 = send(jnp.where(is0, op7, op6), up, down)
    op9 = send(op6, mirror)
    hb = both(ha, other_core)
    s1 = jnp.where(is0, op7, o0)
    s2 = jnp.where(is0, op9, op2)

    ba, ea = label_entries(jnp.concatenate([labels, l1]), vocab_index, z, y, core)
    bb, eb = label_entries(jnp.concatenate([l2, l3]), vocab_index, z, y, core)
    bounds = jnp.stack([ba, bb])
    entries = jnp.stack([ea, eb])

    f32 = jnp.float32
    state = (
        jax.ShapeDtypeStruct((WINDOWS // 2, 8, TILE), f32),
        jax.ShapeDtypeStruct((WINDOWS // 2, 8, TILE), f32),
        jax.ShapeDtypeStruct((2, 8 * 128 + GROUP, 128), f32),
    )
    logits_scratch = pltpu.VMEM((WINDOWS, BLOCK, 128), f32)

    def call(kernel, out_shape, operands, pairs, gflop, limit, extra=()):
        return pl.pallas_call(
            kernel,
            out_shape=out_shape,
            in_specs=[SMEM, SMEM, *([VMEM] * len(operands))],
            out_specs=[VMEM] * len(out_shape),
            scratch_shapes=[*extra, pltpu.VMEM((pairs * BLOCK, width), jnp.bfloat16), logits_scratch],
            cost_estimate=pl.CostEstimate(flops=int(gflop * 1e9), bytes_accessed=0, transcendentals=0),
            compiler_params=pltpu.CompilerParams(vmem_limit_bytes=limit * 2**20),
        )(bounds, entries, *operands)

    early_windows = 2 * EARLY // 128
    ma = call(first_kernel, state, (op1, op3, fa, fb), 1, 4, 8)
    ma = call(second_kernel, state, (op4, op5, fa, fb, *ma), 1, 4, 8)
    mb = call(
        beside_kernel, state, (op1, op3, op4, op5, ga, gb), 2, 4, 14, [pltpu.VMEM((early_windows, 2 * BLOCK, 128), f32)]
    )
    states = (*ma, *mb)
    states = call(
        third_kernel,
        state + state,
        (op1, op3, op4, op5, op6, s1, fa, fb, ga, gb, ha, hb, *states),
        3,
        8,
        16,
        [
            pltpu.VMEM((early_windows, BLOCK, 128), f32),
            pltpu.VMEM((WINDOWS - early_windows, 3 * BLOCK, 128), f32),
        ],
    )
    packed = jax.ShapeDtypeStruct((8, 144, TILE), jnp.bfloat16)
    kept, given = call(
        last_kernel,
        (packed, packed),
        (op8, s2, fa, fb, ga, gb, ha, hb, *states),
        1,
        6,
        16,
        [
            *(pltpu.VMEM(leaf.shape, leaf.dtype) for leaf in state + state),
            pltpu.VMEM((WINDOWS, 8, 128), f32),
            logits_scratch,
        ],
    )
    taken = both(given, other_core)
    sent = pl.pallas_call(
        join_kernel,
        out_shape=jax.ShapeDtypeStruct((8, 224, 128), jnp.bfloat16),
        in_specs=[SMEM, VMEM, VMEM],
        out_specs=VMEM,
        compiler_params=pltpu.CompilerParams(vmem_limit_bytes=8 * 2**20),
    )((y % 2)[None], kept, taken)
    vocabs = lax.axis_size("vocab")
    owners = [
        [rec_index(z, y + side, core) * vocabs + v for side in range(2) for v in range(vocabs)]
        for z in range(NZ)
        for y in range(0, NY, 2)
        for core in range(2)
    ]
    got = lax.all_to_all(sent, ("rec", "vocab"), 0, 0, tiled=True, axis_index_groups=owners)
    log_prob, path = pl.pallas_call(
        align_kernel,
        out_shape=[jax.ShapeDtypeStruct((frames, 128), f32), jax.ShapeDtypeStruct((1,), f32)],
        in_specs=[SMEM, VMEM],
        out_specs=[VMEM, SMEM],
        scratch_shapes=[pltpu.VMEM((DEPTH, frames, 128), f32), pltpu.VMEM((frames, 128), f32)],
        compiler_params=pltpu.CompilerParams(vmem_limit_bytes=8 * 2**20),
    )(jnp.concatenate([audio_len, transcript_len]), got)
    return log_prob[None], path


def solution(mesh):
    placed = (
        P("rec", None, None),
        P(None, ("vocab", "rec")),
        P("rec", None),
        P(("rec", "vocab")),
        P(("rec", "vocab")),
    )

    return jax.shard_map(
        body,
        mesh=mesh,
        in_specs=placed,
        out_specs=(P(("rec", "vocab"), None, None), P(("rec", "vocab"))),
        check_vma=False,
    )
```
